256 devices in a mesh: ctx: 32 (over z, x), tp: 8 (over y, core).
Axes of the slice: x: 4, y: 4, z: 8, core: 2. Of those that a mesh axis runs over, the one named last changes fastest.
Arguments:
- q_nope: bfloat16 [32, 128, 128], P('ctx', 'tp'), may hold values from -6 to 6
- q_rope: bfloat16 [32, 128, 64], P('ctx', 'tp'), may hold values from -256 to 256
- w_uk: bfloat16 [128, 128, 512], P('tp'), may hold values from -0.5 to 0.5
- w_uv: bfloat16 [128, 512, 128], P('tp'), may hold values from -3 to 3
- w_out: bfloat16 [16384, 7168], P('tp', 'ctx'), may hold values from -0.046875 to 0.046875
- prefix_cache: bfloat16 [131072, 576], P('ctx'), may hold values from -6 to 6
- block_table: int32 [2048], P('ctx'), may hold values from 0 to 2047, each once
- prefix_len: int32 [32], replicated, may hold values from 32768 to 131072
- suffix_cache: bfloat16 [32, 256, 576], P('ctx'), may hold values from -12 to 12
- suffix_len: int32 [32], P('ctx'), may hold values from 2 to 256
Outputs:
- layer_out: bfloat16 [32, 7168], P('tp', 'ctx')
The draws below stay inside these ranges and needn't reach their ends.
Inputs may be any that keep to these rules, and one draw needn't show every extreme that they name: A permutation: slots b * 64 to b * 64 + 63 of prefix_cache hold prefix positions block_table[b] * 64 onwards.
All inputs are finite; a program needn't handle non-finite values.
Results may differ from the reference program's by a relative error of at most 0.0078.
Values may be sent and summed in bfloat16 or wider, within the bound.
No kernel may reach another device: no remote copies, remote signals or barrier semaphores. Data moves between devices by JAX's collectives and lax.ppermute only.
A program may use at most 64 MiB of HBM per device.

```python
import jax
import jax.numpy as jnp
from jax import lax

H = 128
LAT = 512
ROPE = 64
NOPE = 128
VDIM = 128
D = 7168
TOK_DEV = 4096
BLOCK = 64
SUF = 256
REQUESTS = 32
NPRE = 131072
NBLK = 2048
N_CTX = 32


def shared_base(key):
    return jax.random.normal(jax.random.fold_in(key, 11), (REQUESTS, ROPE), jnp.float32)


def suffix_rope_part(key):
    noise = jax.random.normal(jax.random.fold_in(key, 13), (REQUESTS, SUF, ROPE), jnp.float32)
    return shared_base(key)[:, None, :] + noise


def draw_suffix_cache(key, part):
    latent = jax.random.normal(jax.random.fold_in(key, 12), (REQUESTS, SUF, LAT), jnp.float32)
    rope = suffix_rope_part(key)
    return jnp.clip(jnp.concatenate([latent, rope], axis=2), -12.0, 12.0).astype(jnp.bfloat16)


def draw_q_rope(key, part):
    noise = jax.random.normal(jax.random.fold_in(key, 21), (REQUESTS, H, ROPE), jnp.float32)
    query = shared_base(key)[:, None, :] + noise
    return jnp.clip(query, -256.0, 256.0).astype(jnp.bfloat16)


def set_ends(drawn, stream_key, low, top_value):
    longest = drawn.shape.index(max(drawn.shape))
    spots = []
    for shift in (0, 1):
        where = [jax.random.randint(jax.random.fold_in(stream_key, axis), (), 0, length) for axis, length in enumerate(drawn.shape)]
        where[longest] = (where[longest] + shift) % drawn.shape[longest]
        spots.append(tuple(where))
    return drawn.at[spots[0]].set(low).at[spots[1]].set(top_value)


def block_scale(stream_key, dims, split, low, high):
    def one(axis_at, blocks):
        steps = jax.random.uniform(jax.random.fold_in(jax.random.fold_in(stream_key, 6), axis_at), (blocks,), jnp.float32, low / len(split), high / len(split))
        return jnp.repeat(jnp.exp(steps), dims[axis_at] // blocks).reshape((-1,) + (1,) * (len(dims) - axis_at - 1))

    level = one(*split[0])
    for cut in split[1:]:
        level = level * one(*cut)
    return level


def normal_values(own_key, shape, scale, bound, split=(), held_as=jnp.bfloat16):
    entries = scale * jax.random.normal(own_key, shape, jnp.float32)
    if split:
        entries = entries * block_scale(own_key, shape, split, -0.22, 0.18)
    return jnp.clip(entries, -bound, bound).astype(held_as)


def setup_inputs(seed: int = 0) -> dict:
    streams_of = jax.random.split(jax.random.key(seed), 11)
    q_nope = normal_values(streams_of[0], (REQUESTS, H, NOPE), 1.0, 6.0, ((0, 32), (1, 8)))
    q_rope = draw_q_rope(jax.random.fold_in(streams_of[10], 71), 0)
    w_uk = normal_values(streams_of[2], (H, NOPE, LAT), NOPE ** -0.5, 0.5, ((0, 8),))
    w_uv = normal_values(streams_of[3], (H, LAT, VDIM), 0.5, 3.0, ((0, 8),))
    w_out = normal_values(streams_of[4], (H * VDIM, D), (H * VDIM) ** -0.5, 0.046875, ((0, 8), (1, 32)))
    prefix_cache = normal_values(streams_of[5], (NPRE, LAT + ROPE), 1.0, 6.0, ((0, 32),))
    block_table = jax.random.permutation(streams_of[6], NBLK).astype(jnp.int32)
    prefix_len = set_ends(jax.random.randint(streams_of[7], (REQUESTS,), NPRE // 4, NPRE + 1), jax.random.fold_in(streams_of[7], 1), NPRE // 4, NPRE).astype(jnp.int32)
    suffix_cache = draw_suffix_cache(jax.random.fold_in(streams_of[10], 71), 0)
    suffix_len = set_ends(jax.random.randint(streams_of[9], (REQUESTS,), 2, SUF + 1), jax.random.fold_in(streams_of[9], 1), 2, SUF).astype(jnp.int32)
    return {"q_nope": q_nope, "q_rope": q_rope, "w_uk": w_uk, "w_uv": w_uv, "w_out": w_out, "prefix_cache": prefix_cache, "block_table": block_table, "prefix_len": prefix_len, "suffix_cache": suffix_cache, "suffix_len": suffix_len}


masked_value = -1e30


def summarize(scores, visible, values, pattern):
    row_peak = jnp.max(jnp.where(visible, scores, masked_value), axis=2)
    weights = jnp.where(visible, jnp.exp(scores - row_peak[:, :, None]), 0.0).astype(jnp.bfloat16)
    weights = lax.optimization_barrier(weights).astype(jnp.float32)
    return row_peak, jnp.sum(weights, axis=2), jnp.einsum(pattern, weights, values)


def reference(q_nope, q_rope, w_uk, w_uv, w_out, prefix_cache, block_table, prefix_len, suffix_cache, suffix_len):
    softmax_scale = (NOPE + ROPE) ** -0.5
    q_latent = jnp.einsum("rhn,hnc->rhc", q_nope.astype(jnp.float32), w_uk.astype(jnp.float32)).astype(jnp.bfloat16)
    joined = lax.optimization_barrier(jnp.concatenate([q_latent, q_rope], axis=2)).astype(jnp.float32)
    positions = (block_table[:, None] * BLOCK + jnp.arange(BLOCK, dtype=jnp.int32)[None, :]).reshape(N_CTX, TOK_DEV)
    segments = prefix_cache.reshape(N_CTX, TOK_DEV, LAT + ROPE)

    def segment_part(pieces):
        block_cache, block_positions = pieces
        cache_wide = block_cache.astype(jnp.float32)
        scores = jnp.einsum("rhc,tc->rht", joined, cache_wide) * softmax_scale
        visible = (block_positions[None, :] < prefix_len[:, None])[:, None, :]
        return summarize(scores, visible, cache_wide[:, :LAT], "rht,tc->rhc")

    seg_peak, seg_mass, seg_weighted = lax.map(segment_part, (segments, positions))
    suffix_wide = suffix_cache.astype(jnp.float32)
    suffix_scores = jnp.einsum("rhc,rtc->rht", joined, suffix_wide) * softmax_scale
    suffix_slots = jnp.arange(SUF, dtype=jnp.int32)
    suffix_visible = (suffix_slots[None, :] < suffix_len[:, None])[:, None, :]
    tail_peak, tail_mass, tail_weighted = summarize(suffix_scores, suffix_visible, suffix_wide[:, :, :LAT], "rht,rtc->rhc")
    highest = jnp.maximum(jnp.max(seg_peak, axis=0), tail_peak)
    factors = jnp.exp(seg_peak - highest[None])
    tail_factor = jnp.exp(tail_peak - highest)
    total_mass = jnp.sum(factors * seg_mass, axis=0) + tail_factor * tail_mass
    total_weighted = jnp.sum(factors[..., None] * seg_weighted, axis=0) + tail_factor[:, :, None] * tail_weighted
    attention = total_weighted / total_mass[:, :, None]
    head_values = jnp.einsum("rhc,hcv->rhv", attention, w_uv.astype(jnp.float32), precision=lax.Precision.HIGHEST).astype(jnp.bfloat16)
    flat_values = head_values.reshape(REQUESTS, H * VDIM)
    return jnp.dot(flat_values, w_out, preferred_element_type=jnp.float32).astype(jnp.bfloat16)
```

```python
import math

import jax
import jax.numpy as jnp
from jax import lax
from jax.sharding import PartitionSpec as P

LAT = 512
ROPE = 64
NOPE = 128
BLOCK = 64


masked_value = -1e30


def sent_to_all(value, axis):
    length = lax.axis_size(axis)
    return lax.all_to_all(
        jnp.broadcast_to(value[None], (length, *value.shape)), axis, 0, 0, tiled=True
    )


def joined_along(pieces, dim):
    shape = list(pieces.shape[1:])
    shape[dim] *= pieces.shape[0]
    return jnp.moveaxis(pieces, 0, dim).reshape(shape)


def collect(value, axis, dim):
    pieces = sent_to_all(value, axis)
    return joined_along(pieces, dim)


def in_one_piece(arrays, axis, split_dim, concat_dim, along):
    widths = [math.prod(a.shape[along:]) for a in arrays]
    both = jnp.concatenate(
        [a.reshape(*a.shape[:along], w) for a, w in zip(arrays, widths)], axis=along
    )
    out = lax.all_to_all(both, axis, split_axis=split_dim, concat_axis=concat_dim, tiled=True)
    pieces = jnp.split(out, [sum(widths[:k]) for k in range(1, len(widths))], axis=along)
    return tuple((b.reshape(*out.shape[:along], *a.shape[along:]) for a, b in zip(arrays, pieces)))


def split_up(value, dim, length):
    shape = value.shape
    pieces = value.reshape(*shape[:dim], length, shape[dim] // length, *shape[dim + 1 :])
    return jnp.moveaxis(pieces, dim, 0)


def sent_and_summed(value, axis, dim):
    pieces = split_up(value, dim, lax.axis_size(axis))
    arrived = lax.all_to_all(pieces, axis, split_axis=0, concat_axis=0, tiled=True)
    return arrived.sum(axis=0)


def partial_stats(scores, visible, values, pattern):
    row_peak = jnp.max(jnp.where(visible, scores, masked_value), axis=2)
    weights = jnp.where(visible, jnp.exp(scores - row_peak[:, :, None]), 0.0).astype(jnp.bfloat16)
    row_mass = jnp.sum(weights, axis=2, dtype=jnp.float32)
    row_weighted = jnp.einsum(pattern, weights, values, preferred_element_type=jnp.float32)
    return (row_peak, row_mass, row_weighted)


def value_project(latent, value_weight):
    high = latent.astype(jnp.bfloat16)
    low = (latent - high.astype(jnp.float32)).astype(jnp.bfloat16)
    parts = jnp.stack([high, low])
    return jnp.einsum("prhc,hcv->prhv", parts, value_weight, preferred_element_type=jnp.float32).sum(axis=0)


def on_device(
    q_nope,
    q_rope,
    w_uk,
    w_uv,
    w_out,
    prefix_cache,
    block_table,
    prefix_len,
    suffix_cache,
    suffix_len,
):
    softmax_scale = (NOPE + ROPE) ** (-0.5)
    raw_queries = collect(jnp.concatenate([q_nope, q_rope], axis=2), "ctx", 0)

    def absorb(nope, rope):
        latent = jnp.einsum("rhn,hnc->rhc", nope, w_uk, preferred_element_type=jnp.float32)
        return jnp.concatenate([latent.astype(jnp.bfloat16), rope], axis=2)

    own_queries = absorb(q_nope, q_rope)
    all_queries = absorb(raw_queries[:, :, :NOPE], raw_queries[:, :, NOPE:])
    ctx_count = lax.axis_size("ctx")
    own_count = own_queries.shape[0]
    positions = (
        block_table[:, None] * BLOCK + jnp.arange(BLOCK, dtype=jnp.int32)[None, :]
    ).reshape(-1)
    visible = (positions[None, :] < prefix_len[:, None])[:, None, :]
    scores = (
        jnp.einsum("rhc,tc->rht", all_queries, prefix_cache, preferred_element_type=jnp.float32)
        * softmax_scale
    )
    row_peak, row_mass, row_weighted = partial_stats(
        scores, visible, prefix_cache[:, :LAT], "rht,tc->rhc"
    )
    row_weighted = value_project(row_weighted, w_uv)
    suffix_scores = (
        jnp.einsum("rhc,rtc->rht", own_queries, suffix_cache, preferred_element_type=jnp.float32)
        * softmax_scale
    )
    suffix_slots = jnp.arange(suffix_cache.shape[1], dtype=jnp.int32)
    suffix_visible = (suffix_slots[None, :] < suffix_len[:, None])[:, None, :]
    tail_peak, tail_mass, tail_weighted = partial_stats(
        suffix_scores, suffix_visible, suffix_cache[:, :, :LAT], "rht,rtc->rhc"
    )
    tail_weighted = value_project(tail_weighted, w_uv)

    def by_owner(values):
        return values.reshape((ctx_count, own_count) + values.shape[1:])

    got_peak, got_mass, got_weighted = in_one_piece(
        (by_owner(row_peak), by_owner(row_mass), by_owner(row_weighted)), "ctx", 0, 0, 3
    )
    highest = jnp.maximum(jnp.max(got_peak, axis=0), tail_peak)
    factors = jnp.exp(got_peak - highest[None])
    tail_factor = jnp.exp(tail_peak - highest)
    total_mass = jnp.sum(factors * got_mass, axis=0) + tail_factor * tail_mass
    total_weighted = (
        jnp.sum(factors[..., None] * got_weighted, axis=0) + tail_factor[:, :, None] * tail_weighted
    )
    head_values = (total_weighted / total_mass[:, :, None]).astype(jnp.bfloat16)
    flat_values = head_values.reshape(own_count, -1)
    every_value = collect(flat_values, "ctx", 0)
    return sent_and_summed(
        jnp.dot(every_value, w_out, preferred_element_type=jnp.float32), "tp", 0
    ).astype(jnp.bfloat16)


def solution(mesh):
    placed = (
        P("ctx", "tp", None),
        P("ctx", "tp", None),
        P("tp", None, None),
        P("tp", None, None),
        P("tp", "ctx"),
        P("ctx", None),
        P("ctx"),
        P(),
        P("ctx", None, None),
        P("ctx"),
    )
    return jax.shard_map(
        on_device, mesh=mesh, in_specs=placed, out_specs=P("tp", "ctx"), check_vma=False
    )
```

```python
import functools
import math

import jax
import jax.numpy as jnp
from jax import lax
from jax.experimental import pallas as pl
from jax.experimental.pallas import tpu as pltpu
from jax.sharding import PartitionSpec as P

LAT = 512
ROPE = 64
NOPE = 128
BLOCK = 64
LANES = 128
ROWS = 24
NEG = -1e30
LOG2E = math.log2(math.e)


def segment_kernel(q_ref, w_uk_ref, pos_ref, len_ref, cache_ref, w_uv_ref, out_ref,
                   q32, query, cache, w_uv, scores, packed, cache_sems, w_sem, *, chunks, log_scale):
    requests=len_ref.shape[0]
    heads=w_uk_ref.shape[0]
    slots=cache.shape[1]
    width=slots//chunks
    def fetch(j):
        at=pl.ds(j*width,width)
        return pltpu.make_async_copy(cache_ref.at[:,at], cache.at[pl.ds(0,LAT+ROPE),at], cache_sems.at[j])
    for j in range(chunks): fetch(j).start()
    w_copy=pltpu.make_async_copy(w_uv_ref,w_uv,w_sem)
    w_copy.start()
    q32[...]=q_ref[...].astype(jnp.float32)
    cache[LAT+ROPE:,:]=jnp.zeros((cache.shape[0]-LAT-ROPE,slots),jnp.bfloat16)
    lane=lax.broadcasted_iota(jnp.int32,(requests,128),1)
    for h in range(heads):
        nope=q32[pl.ds(h,requests,stride=ROWS),:].astype(jnp.bfloat16)
        latent=jnp.dot(nope,w_uk_ref[h],preferred_element_type=jnp.float32).astype(jnp.bfloat16)
        rope=q32[pl.ds(16+h%8,requests,stride=ROWS),:]
        if h>=8: rope=pltpu.roll(rope,64,1)
        rope=jnp.where(lane<ROPE,rope,0.0).astype(jnp.bfloat16)
        query[h*requests:(h+1)*requests,:LAT]=latent
        query[h*requests:(h+1)*requests,LAT:]=rope
    rows=heads*requests
    top=None
    for j in range(chunks):
        fetch(j).wait()
        at=slice(j*width,(j+1)*width)
        s=jnp.dot(query[...],cache[:,at],preferred_element_type=jnp.float32)
        bias=jnp.where(pos_ref[:,at]<len_ref[...],0.0,NEG)
        s=(s.reshape(heads,requests,width)*log_scale+bias[None]).reshape(rows,width)
        scores[:,at]=s
        m=jnp.max(s,axis=1,keepdims=True)
        top=m if top is None else jnp.maximum(top,m)
    mass=None
    acc=None
    for j in range(chunks):
        at=slice(j*width,(j+1)*width)
        p=jnp.exp2(scores[:,at]-top)
        pb=p.astype(jnp.bfloat16)
        l=jnp.sum(p,axis=1,keepdims=True)
        o=lax.dot_general(pb,cache[:LAT,at],(((1,),(1,)),((),())),preferred_element_type=jnp.float32)
        mass=l if mass is None else mass+l
        acc=o if acc is None else acc+o
    w_copy.wait()
    high=acc.astype(jnp.bfloat16)
    low=(acc-high.astype(jnp.float32)).astype(jnp.bfloat16)
    peak_tile=jnp.zeros((requests,128),jnp.float32)
    mass_tile=jnp.zeros((requests,128),jnp.float32)
    packed[...]=jnp.zeros(packed.shape,jnp.float32)
    for h in range(heads):
        r=slice(h*requests,(h+1)*requests)
        both=jnp.concatenate([high[r],low[r]],axis=0)
        v=jnp.dot(both,w_uv[h],preferred_element_type=jnp.float32)
        packed[pl.ds(h,requests,stride=ROWS),:]=v[:requests]+v[requests:]
        peak_tile=jnp.where(lane==h,top[r],peak_tile)
        mass_tile=jnp.where(lane==h,mass[r],mass_tile)
    def parts(x,n):
        got=[]
        for _ in range(n):
            t=x.astype(jnp.bfloat16).astype(jnp.float32)
            got.append(t); x=x-t
        return got
    stats=None
    for k,t in enumerate(parts(peak_tile,3)+parts(mass_tile,2)):
        t=pltpu.roll(t,16*k,1) if k else t
        stats=t if stats is None else stats+t
    packed[pl.ds(heads,requests,stride=ROWS),:]=stats
    out_ref[...]=packed[...].astype(jnp.bfloat16)


def segment(q,w_uk,pos,lens,cacheT,w_uv,chunks=4):
    heads=w_uk.shape[0]; requests=lens.shape[0]; slots=cacheT.shape[1]
    rows=heads*requests
    vm=pl.BlockSpec(memory_space=pltpu.VMEM); hbm=pl.BlockSpec(memory_space=pltpu.HBM)
    return pl.pallas_call(
        functools.partial(segment_kernel,chunks=chunks,log_scale=(NOPE+ROPE)**-0.5*math.log2(math.e)),
        out_shape=jax.ShapeDtypeStruct((requests*ROWS,128),jnp.bfloat16),
        in_specs=[vm,vm,vm,vm,hbm,hbm], out_specs=vm,
        scratch_shapes=[pltpu.VMEM((requests*ROWS,128),jnp.float32),pltpu.VMEM((rows,640),jnp.bfloat16),
            pltpu.VMEM((640,slots),jnp.bfloat16),pltpu.VMEM(w_uv.shape,jnp.bfloat16),
            pltpu.VMEM((rows,slots),jnp.float32),pltpu.VMEM((requests*ROWS,128),jnp.float32),
            pltpu.SemaphoreType.DMA((chunks,)),pltpu.SemaphoreType.DMA],
        compiler_params=pltpu.CompilerParams(vmem_limit_bytes=50 * 1024 * 1024),
        name="segment",
    )(q,w_uk,pos,lens,cacheT,w_uv)


def combine_kernel(got_ref, tail_ref, tail_stats_ref, out_ref, got32, *, heads, sources):
    got32[...] = got_ref[...].astype(jnp.float32)
    stats = got32[pl.ds(heads, sources, stride=ROWS), :]

    def part(first, count):
        terms = [pltpu.roll(stats, (LANES - 16 * k) % LANES, 1) if k else stats for k in range(first, first + count)]
        return sum(terms[1:], terms[0])

    peak = part(0, 3)
    mass = part(3, 2)
    tail_peak = tail_stats_ref[0:1, :]
    tail_mass = tail_stats_ref[1:2, :]
    highest = jnp.maximum(jnp.max(peak, axis=0, keepdims=True), tail_peak)
    factor = jnp.exp2(peak - highest)
    tail_factor = jnp.exp2(tail_peak - highest)
    total = jnp.sum(factor * mass, axis=0, keepdims=True) + tail_factor * tail_mass
    lane = lax.broadcasted_iota(jnp.int32, total.shape, 1)
    total = jnp.where(lane < heads, total, 1.0)
    share = jnp.concatenate(
        [
            factor / total,
            jnp.broadcast_to(tail_factor / total, (8, LANES)),
            jnp.zeros((LANES - sources - 8, LANES), jnp.float32),
        ],
        axis=0,
    )
    share = share.T[:heads]
    value = tail_ref[...] * share[:, sources : sources + 1]
    for s in range(sources):
        value = value + got32[s * ROWS : s * ROWS + heads, :] * share[:, s : s + 1]
    value = value.astype(jnp.bfloat16)
    for s in range(sources):
        out_ref[s * heads : (s + 1) * heads, :] = value


def combine(got, tail, tail_stats, sources):
    heads = tail.shape[0]
    return pl.pallas_call(
        functools.partial(combine_kernel, heads=heads, sources=sources),
        out_shape=jax.ShapeDtypeStruct((sources * heads, LANES), jnp.bfloat16),
        in_specs=[pl.BlockSpec(memory_space=pltpu.VMEM)] * 3,
        out_specs=pl.BlockSpec(memory_space=pltpu.VMEM),
        scratch_shapes=[pltpu.VMEM((sources * ROWS, LANES), jnp.float32)],
        compiler_params=pltpu.CompilerParams(vmem_limit_bytes=8 * 1024 * 1024),
        name="combine",
    )(got, tail, tail_stats)


def output_kernel(values_ref, w_ref, out_ref, values32, flat, *, heads, requests):
    values32[...] = values_ref[...].astype(jnp.float32)
    for h in range(heads):
        flat[:, h * LANES : (h + 1) * LANES] = values32[pl.ds(h, requests, stride=heads), :].astype(
            jnp.bfloat16
        )
    out_ref[...] = lax.dot_general(
        flat[...], w_ref[...], (((1,), (1,)), ((), ())), preferred_element_type=jnp.float32
    )


def output_product(values, w_out_t, requests):
    heads = values.shape[0] // requests
    return pl.pallas_call(
        functools.partial(output_kernel, heads=heads, requests=requests),
        out_shape=jax.ShapeDtypeStruct((requests, w_out_t.shape[0]), jnp.float32),
        in_specs=[pl.BlockSpec(memory_space=pltpu.VMEM)] * 2,
        out_specs=pl.BlockSpec(memory_space=pltpu.VMEM),
        scratch_shapes=[
            pltpu.VMEM(values.shape, jnp.float32),
            pltpu.VMEM((requests, heads * LANES), jnp.bfloat16),
        ],
        compiler_params=pltpu.CompilerParams(vmem_limit_bytes=8 * 1024 * 1024),
        name="output_product",
    )(values, w_out_t)


def spread(block, axis):
    count = lax.axis_size(axis)
    return lax.all_to_all(
        jnp.broadcast_to(block[None], (count, *block.shape)), axis, 0, 0, tiled=True
    )


def tail_part(q_nope, q_rope, w_uk, w_uv, suffix, suffix_len):
    latent = jnp.einsum("hn,hnc->hc", q_nope, w_uk, preferred_element_type=jnp.float32)
    query = jnp.concatenate([latent.astype(jnp.bfloat16), q_rope], axis=1)
    scores = jnp.einsum("hc,tc->ht", query, suffix, preferred_element_type=jnp.float32)
    scores = scores * ((NOPE + ROPE) ** -0.5)
    visible = (jnp.arange(suffix.shape[0], dtype=jnp.int32) < suffix_len)[None, :]
    peak = jnp.max(jnp.where(visible, scores, NEG), axis=1)
    weights = jnp.where(visible, jnp.exp(scores - peak[:, None]), 0.0).astype(jnp.bfloat16)
    mass = jnp.sum(weights, axis=1, dtype=jnp.float32)
    weighted = jnp.einsum("ht,tc->hc", weights, suffix[:, :LAT], preferred_element_type=jnp.float32)
    high = weighted.astype(jnp.bfloat16)
    low = (weighted - high.astype(jnp.float32)).astype(jnp.bfloat16)
    value = jnp.einsum(
        "phc,hcv->phv", jnp.stack([high, low]), w_uv, preferred_element_type=jnp.float32
    ).sum(axis=0)
    stats = jnp.pad(jnp.stack([peak * LOG2E, mass]), ((0, 6), (0, LANES - peak.shape[0])))
    return value, stats


def on_device(
    q_nope,
    q_rope,
    w_uk,
    w_uv,
    w_out,
    prefix_cache,
    block_table,
    prefix_len,
    suffix_cache,
    suffix_len,
):
    requests = prefix_len.shape[0]
    heads = w_uk.shape[0]
    half = heads // 2
    rope_pairs = jnp.concatenate([q_rope[0, :half], q_rope[0, half:]], axis=1)
    raw = spread(jnp.concatenate([q_nope[0], rope_pairs], axis=0), "ctx")
    positions = (
        block_table[:, None] * BLOCK + jnp.arange(BLOCK, dtype=jnp.int32)[None, :]
    ).reshape(1, -1)
    packed = segment(
        raw.reshape(requests * ROWS, LANES),
        w_uk,
        positions,
        prefix_len[:, None],
        prefix_cache.T,
        w_uv,
    )
    got = lax.all_to_all(packed.reshape(requests, ROWS, LANES), "ctx", 0, 0, tiled=True)
    tail, tail_stats = tail_part(
        q_nope[0], q_rope[0], w_uk, w_uv, suffix_cache[0], suffix_len
    )
    values = combine(got.reshape(requests * ROWS, LANES), tail, tail_stats, requests)
    every = lax.all_to_all(values.reshape(requests, heads, LANES), "ctx", 0, 0, tiled=True)
    partial = output_product(every.reshape(requests * heads, LANES), w_out.T, requests)
    tp = lax.axis_size("tp")
    pieces = lax.all_to_all(
        partial.reshape(tp, requests // tp, -1), "tp", 0, 0, tiled=True
    )
    return pieces.sum(axis=0).astype(jnp.bfloat16)


def solution(mesh):
    placed = (
        P("ctx", "tp", None),
        P("ctx", "tp", None),
        P("tp", None, None),
        P("tp", None, None),
        P("tp", "ctx"),
        P("ctx", None),
        P("ctx"),
        P(),
        P("ctx", None, None),
        P("ctx"),
    )
    return jax.shard_map(
        on_device, mesh=mesh, in_specs=placed, out_specs=P("tp", "ctx"), check_vma=False
    )
```

```python
import functools
import math

import jax
import jax.numpy as jnp
from jax import lax
from jax.experimental import pallas as pl
from jax.experimental.pallas import tpu as pltpu
from jax.sharding import PartitionSpec as P

LAT = 512
ROPE = 64
NOPE = 128
BLOCK = 64
LANES = 128
ROWS = 24
NEG = -1e30
WHOLE_VMEM = 60 * 1024 * 1024
SCALE = (NOPE + ROPE) ** -0.5 * math.log2(math.e)


def segment_kernel(
    q_ref,
    w_uk_ref,
    pos_ref,
    len_ref,
    cache_ref,
    w_uv_ref,
    out_ref,
    q32,
    query,
    cache,
    w_uv,
    packed,
    cache_sems,
    w_sem,
    *,
    pieces,
):
    requests = len_ref.shape[0]
    heads = w_uk_ref.shape[0]
    half = heads // 2
    rows = heads * requests
    width = cache.shape[1] // sum(pieces)
    firsts = [sum(pieces[:k]) for k in range(len(pieces))]

    def piece(k):
        at = pl.ds(firsts[k] * width, pieces[k] * width)
        return pltpu.make_async_copy(
            cache_ref.at[:, at], cache.at[pl.ds(0, LAT + ROPE), at], cache_sems.at[k]
        )

    for k in range(len(pieces)):
        piece(k).start()
    w_copy = pltpu.make_async_copy(w_uv_ref, w_uv, w_sem)
    w_copy.start()

    q32[...] = q_ref[...].astype(jnp.float32)
    cache[LAT + ROPE :, :] = jnp.zeros((cache.shape[0] - LAT - ROPE, cache.shape[1]), jnp.bfloat16)
    lane = lax.broadcasted_iota(jnp.int32, (requests, LANES), 1)
    for h in range(heads):
        at = slice(h * requests, (h + 1) * requests)
        nope = q32[pl.ds(h, requests, stride=ROWS), :].astype(jnp.bfloat16)
        latent = jnp.dot(nope, w_uk_ref[h], preferred_element_type=jnp.float32)
        rope = q32[pl.ds(heads + h % half, requests, stride=ROWS), :]
        if h >= half:
            rope = pltpu.roll(rope, LANES - ROPE, 1)
        query[at, :LAT] = latent.astype(jnp.bfloat16)
        query[at, LAT:] = jnp.where(lane < ROPE, rope, 0.0).astype(jnp.bfloat16)

    peak = mass = total = None

    def take(at, scores):
        nonlocal peak, mass, total
        highest = jnp.max(scores, axis=1, keepdims=True)
        if peak is not None:
            highest = jnp.maximum(peak, highest)
        weights = jnp.exp2(scores - highest)
        part = jnp.sum(weights, axis=1, keepdims=True)
        values = lax.dot_general(
            weights.astype(jnp.bfloat16),
            cache[:LAT, at],
            (((1,), (1,)), ((), ())),
            preferred_element_type=jnp.float32,
        )
        if peak is None:
            mass, total = part, values
        else:
            keep = jnp.exp2(peak - highest)
            mass, total = mass * keep + part, total * keep + values
        peak = highest

    waiting = None
    for j in range(sum(pieces)):
        if j in firsts:
            piece(firsts.index(j)).wait()
            if j == firsts[-1]:
                w_copy.wait()
        at = slice(j * width, (j + 1) * width)
        scores = jnp.dot(query[...], cache[:, at], preferred_element_type=jnp.float32)
        hidden = jnp.where(pos_ref[:, at] < len_ref[...], 0.0, NEG)
        scores = scores.reshape(heads, requests, width) * SCALE + hidden[None]
        if waiting is not None:
            take(*waiting)
        waiting = (at, scores.reshape(rows, width))
    take(*waiting)

    high = total.astype(jnp.bfloat16)
    low = (total - high.astype(jnp.float32)).astype(jnp.bfloat16)
    peaks = jnp.zeros((requests, LANES), jnp.float32)
    masses = jnp.zeros((requests, LANES), jnp.float32)
    packed[...] = jnp.zeros(packed.shape, jnp.float32)
    for h in range(heads):
        at = slice(h * requests, (h + 1) * requests)
        both = jnp.concatenate([high[at], low[at]], axis=0)
        value = jnp.dot(both, w_uv[h], preferred_element_type=jnp.float32)
        packed[pl.ds(h, requests, stride=ROWS), :] = value[:requests] + value[requests:]
        peaks = jnp.where(lane == h, peak[at], peaks)
        masses = jnp.where(lane == h, mass[at], masses)

    def terms(x, count):
        found = []
        for _ in range(count):
            term = x.astype(jnp.bfloat16).astype(jnp.float32)
            found.append(term)
            x = x - term
        return found

    stats = None
    for k, term in enumerate(terms(peaks, 3) + terms(masses, 2)):
        term = pltpu.roll(term, 16 * k, 1) if k else term
        stats = term if stats is None else stats + term
    packed[pl.ds(heads, requests, stride=ROWS), :] = stats
    out_ref[...] = packed[...].astype(jnp.bfloat16)


def segment(q, w_uk, positions, lens, cache_t, w_uv, pieces=(2, 6)):
    heads = w_uk.shape[0]
    requests = lens.shape[0]
    vmem = pl.BlockSpec(memory_space=pltpu.VMEM)
    hbm = pl.BlockSpec(memory_space=pltpu.HBM)
    return pl.pallas_call(
        functools.partial(segment_kernel, pieces=pieces),
        out_shape=jax.ShapeDtypeStruct((requests * ROWS, LANES), jnp.bfloat16),
        in_specs=[vmem, vmem, vmem, vmem, hbm, hbm],
        out_specs=vmem,
        scratch_shapes=[
            pltpu.VMEM((requests * ROWS, LANES), jnp.float32),
            pltpu.VMEM((heads * requests, LAT + LANES), jnp.bfloat16),
            pltpu.VMEM((LAT + LANES, cache_t.shape[1]), jnp.bfloat16),
            pltpu.VMEM(w_uv.shape, jnp.bfloat16),
            pltpu.VMEM((requests * ROWS, LANES), jnp.float32),
            pltpu.SemaphoreType.DMA((len(pieces),)),
            pltpu.SemaphoreType.DMA,
        ],
        compiler_params=pltpu.CompilerParams(vmem_limit_bytes=50 * 1024 * 1024),
        name="segment",
    )(q, w_uk, positions, lens, cache_t, w_uv)


def start_fetch(pairs, sems):
    copies = [pltpu.make_async_copy(a, b, sems.at[k]) for k, (a, b) in enumerate(pairs)]
    for copy in copies:
        copy.start()
    return copies


def fetch(pairs, sems):
    for copy in start_fetch(pairs, sems):
        copy.wait()


def pack_kernel(q_nope_hbm, q_rope_hbm, out_ref, q_nope_ref, q_rope_ref, sems):
    fetch([(q_nope_hbm, q_nope_ref), (q_rope_hbm, q_rope_ref)], sems)
    rope = q_rope_ref[...].astype(jnp.float32)
    half = rope.shape[0] // 2
    pairs = jnp.concatenate([rope[:half], rope[half:]], axis=1)
    block = jnp.concatenate([q_nope_ref[...].astype(jnp.float32), pairs], axis=0)
    block = block.astype(jnp.bfloat16)
    out_ref[...] = jnp.broadcast_to(block[None], out_ref.shape)


def pack(q_nope, q_rope, count):
    return pl.pallas_call(
        pack_kernel,
        out_shape=jax.ShapeDtypeStruct((count, ROWS, LANES), jnp.bfloat16),
        in_specs=[pl.BlockSpec(memory_space=pltpu.HBM)] * 2,
        out_specs=pl.BlockSpec(memory_space=pltpu.VMEM),
        scratch_shapes=[
            pltpu.VMEM(q_nope.shape, q_nope.dtype),
            pltpu.VMEM(q_rope.shape, q_rope.dtype),
            pltpu.SemaphoreType.DMA((2,)),
        ],
        compiler_params=pltpu.CompilerParams(vmem_limit_bytes=WHOLE_VMEM),
        name="pack",
    )(q_nope, q_rope)


def tail_kernel(
    q_nope_hbm,
    q_rope_hbm,
    w_uk_hbm,
    w_uv_hbm,
    suffix_hbm,
    len_ref,
    out_ref,
    stats_ref,
    q_nope_ref,
    q_rope_ref,
    w_uk_ref,
    suffix_ref,
    w_uv,
    sems,
):
    copies = start_fetch(
        [
            (q_nope_hbm, q_nope_ref),
            (q_rope_hbm, q_rope_ref),
            (w_uk_hbm, w_uk_ref),
            (suffix_hbm, suffix_ref),
            (w_uv_hbm, w_uv),
        ],
        sems,
    )
    for copy in copies[:-1]:
        copy.wait()
    heads = q_nope_ref.shape[0]

    def spread_heads(x):
        row = lax.broadcasted_iota(jnp.int32, x.shape, 0) % heads
        return jnp.concatenate(
            [jnp.where(row == h, x, 0.0).astype(jnp.bfloat16) for h in range(heads)], axis=1
        )

    latent = jnp.dot(
        spread_heads(q_nope_ref[...].astype(jnp.float32)),
        w_uk_ref[...].reshape(-1, LAT),
        preferred_element_type=jnp.float32,
    ).astype(jnp.bfloat16)
    scores = jnp.dot(latent, suffix_ref[:LAT, :], preferred_element_type=jnp.float32)
    scores = scores + jnp.dot(
        q_rope_ref[...], suffix_ref[LAT:, :], preferred_element_type=jnp.float32
    )
    slot = lax.broadcasted_iota(jnp.int32, scores.shape, 1)
    scores = scores * SCALE + jnp.where(slot < len_ref[0], 0.0, NEG)
    peak = jnp.max(scores, axis=1, keepdims=True)
    weights = jnp.exp2(scores - peak)
    mass = jnp.sum(weights, axis=1, keepdims=True)
    weighted = lax.dot_general(
        weights.astype(jnp.bfloat16),
        suffix_ref[:LAT, :],
        (((1,), (1,)), ((), ())),
        preferred_element_type=jnp.float32,
    )
    high = weighted.astype(jnp.bfloat16).astype(jnp.float32)
    both = spread_heads(jnp.concatenate([high, weighted - high], axis=0))
    copies[-1].wait()
    value = jnp.dot(both, w_uv[...].reshape(-1, LANES), preferred_element_type=jnp.float32)
    out_ref[...] = value[:heads] + value[heads:]
    row = lax.broadcasted_iota(jnp.int32, (heads, LANES), 0)
    lane = lax.broadcasted_iota(jnp.int32, (heads, LANES), 1)
    stats_ref[0:1, :] = jnp.sum(jnp.where(row == lane, peak, 0.0), axis=0, keepdims=True)
    stats_ref[1:2, :] = jnp.sum(jnp.where(row == lane, mass, 0.0), axis=0, keepdims=True)


def tail_part(q_nope, q_rope, w_uk, w_uv, suffix_t, suffix_len):
    vmem = pl.BlockSpec(memory_space=pltpu.VMEM)
    return pl.pallas_call(
        tail_kernel,
        out_shape=(
            jax.ShapeDtypeStruct((q_nope.shape[0], LANES), jnp.float32),
            jax.ShapeDtypeStruct((2, LANES), jnp.float32),
        ),
        in_specs=[pl.BlockSpec(memory_space=pltpu.HBM)] * 5
        + [pl.BlockSpec(memory_space=pltpu.SMEM)],
        out_specs=(vmem, vmem),
        scratch_shapes=[
            pltpu.VMEM(x.shape, x.dtype) for x in (q_nope, q_rope, w_uk, suffix_t, w_uv)
        ]
        + [pltpu.SemaphoreType.DMA((5,))],
        compiler_params=pltpu.CompilerParams(vmem_limit_bytes=WHOLE_VMEM),
        name="tail",
    )(q_nope, q_rope, w_uk, w_uv, suffix_t, suffix_len)


def combine_kernel(got_ref, tail_ref, tail_stats_ref, out_ref, got32, *, heads, sources):
    got32[...] = got_ref[...].astype(jnp.float32)
    stats = got32[pl.ds(heads, sources, stride=ROWS), :]

    def part(first, count):
        terms = [pltpu.roll(stats, (LANES - 16 * k) % LANES, 1) if k else stats for k in range(first, first + count)]
        return sum(terms[1:], terms[0])

    peak = part(0, 3)
    mass = part(3, 2)
    tail_peak = tail_stats_ref[0:1, :]
    tail_mass = tail_stats_ref[1:2, :]
    highest = jnp.maximum(jnp.max(peak, axis=0, keepdims=True), tail_peak)
    factor = jnp.exp2(peak - highest)
    tail_factor = jnp.exp2(tail_peak - highest)
    total = jnp.sum(factor * mass, axis=0, keepdims=True) + tail_factor * tail_mass
    lane = lax.broadcasted_iota(jnp.int32, total.shape, 1)
    total = jnp.where(lane < heads, total, 1.0)
    share = jnp.concatenate(
        [
            factor / total,
            jnp.broadcast_to(tail_factor / total, (8, LANES)),
            jnp.zeros((LANES - sources - 8, LANES), jnp.float32),
        ],
        axis=0,
    )
    share = share.T[:heads]
    value = tail_ref[...] * share[:, sources : sources + 1]
    for s in range(sources):
        value = value + got32[s * ROWS : s * ROWS + heads, :] * share[:, s : s + 1]
    value = value.astype(jnp.bfloat16)
    for s in range(sources):
        out_ref[s * heads : (s + 1) * heads, :] = value


def combine(got, tail, tail_stats, sources):
    heads = tail.shape[0]
    return pl.pallas_call(
        functools.partial(combine_kernel, heads=heads, sources=sources),
        out_shape=jax.ShapeDtypeStruct((sources * heads, LANES), jnp.bfloat16),
        in_specs=[pl.BlockSpec(memory_space=pltpu.VMEM)] * 3,
        out_specs=pl.BlockSpec(memory_space=pltpu.VMEM),
        scratch_shapes=[pltpu.VMEM((sources * ROWS, LANES), jnp.float32)],
        compiler_params=pltpu.CompilerParams(vmem_limit_bytes=8 * 1024 * 1024),
        name="combine",
    )(got, tail, tail_stats)


def output_kernel(values_ref, w_ref, out_ref, values32, flat, *, heads, requests):
    values32[...] = values_ref[...].astype(jnp.float32)
    for h in range(heads):
        flat[:, h * LANES : (h + 1) * LANES] = values32[pl.ds(h, requests, stride=heads), :].astype(
            jnp.bfloat16
        )
    out_ref[...] = lax.dot_general(
        flat[...], w_ref[...], (((1,), (1,)), ((), ())), preferred_element_type=jnp.float32
    )


def output_product(values, w_out_t, requests):
    heads = values.shape[0] // requests
    return pl.pallas_call(
        functools.partial(output_kernel, heads=heads, requests=requests),
        out_shape=jax.ShapeDtypeStruct((requests, w_out_t.shape[0]), jnp.float32),
        in_specs=[pl.BlockSpec(memory_space=pltpu.VMEM)] * 2,
        out_specs=pl.BlockSpec(memory_space=pltpu.VMEM),
        scratch_shapes=[
            pltpu.VMEM(values.shape, jnp.float32),
            pltpu.VMEM((requests, heads * LANES), jnp.bfloat16),
        ],
        compiler_params=pltpu.CompilerParams(vmem_limit_bytes=8 * 1024 * 1024),
        name="output_product",
    )(values, w_out_t)


def on_device(
    q_nope,
    q_rope,
    w_uk,
    w_uv,
    w_out,
    prefix_cache,
    block_table,
    prefix_len,
    suffix_cache,
    suffix_len,
):
    requests = prefix_len.shape[0]
    heads = w_uk.shape[0]
    raw = lax.all_to_all(pack(q_nope[0], q_rope[0], requests), "ctx", 0, 0, tiled=True)
    tail, tail_stats = tail_part(
        q_nope[0], q_rope[0], w_uk, w_uv, suffix_cache[0].T, suffix_len
    )
    positions = (
        block_table[:, None] * BLOCK + jnp.arange(BLOCK, dtype=jnp.int32)[None, :]
    ).reshape(1, -1)
    raw, tail, tail_stats = lax.optimization_barrier((raw, tail, tail_stats))
    packed = segment(
        raw.reshape(requests * ROWS, LANES),
        w_uk,
        positions,
        prefix_len[:, None],
        prefix_cache.T,
        w_uv,
    )
    got = lax.all_to_all(packed.reshape(requests, ROWS, LANES), "ctx", 0, 0, tiled=True)
    values = combine(got.reshape(requests * ROWS, LANES), tail, tail_stats, requests)
    every = lax.all_to_all(values.reshape(requests, heads, LANES), "ctx", 0, 0, tiled=True)
    partial = output_product(every.reshape(requests * heads, LANES), w_out.T, requests)
    tp = lax.axis_size("tp")
    pieces = lax.all_to_all(
        partial.reshape(tp, requests // tp, -1), "tp", 0, 0, tiled=True
    )
    return pieces.sum(axis=0).astype(jnp.bfloat16)


def solution(mesh):
    placed = (
        P("ctx", "tp", None),
        P("ctx", "tp", None),
        P("tp", None, None),
        P("tp", None, None),
        P("tp", "ctx"),
        P("ctx", None),
        P("ctx"),
        P(),
        P("ctx", None, None),
        P("ctx"),
    )
    return jax.shard_map(
        on_device, mesh=mesh, in_specs=placed, out_specs=P("tp", "ctx"), check_vma=False
    )
```

```python
import functools
import math

import jax
import jax.numpy as jnp
from jax import lax
from jax.experimental import pallas as pl
from jax.experimental.pallas import tpu as pltpu
from jax.sharding import PartitionSpec as P

LAT = 512
ROPE = 64
NOPE = 128
BLOCK = 64
LANES = 128
ROWS = 24
NEG = -1e30
CTX_FIRST = 18
TP_FIRST = 4
WHOLE_VMEM = 60 * 1024 * 1024
SCALE = (NOPE + ROPE) ** -0.5 * math.log2(math.e)


def segment_kernel(
    q_ref,
    w_uk_ref,
    pos_ref,
    len_ref,
    cache_ref,
    w_uv_ref,
    out_ref,
    q32,
    query,
    cache,
    w_uv,
    packed,
    cache_sems,
    w_sem,
    *,
    pieces,
):
    requests = len_ref.shape[0]
    heads = w_uk_ref.shape[0]
    half = heads // 2
    rows = heads * requests
    width = cache.shape[1] // sum(pieces)
    firsts = [sum(pieces[:k]) for k in range(len(pieces))]

    def piece(k):
        at = pl.ds(firsts[k] * width, pieces[k] * width)
        return pltpu.make_async_copy(
            cache_ref.at[:, at], cache.at[pl.ds(0, LAT + ROPE), at], cache_sems.at[k]
        )

    for k in range(len(pieces)):
        piece(k).start()
    w_copy = pltpu.make_async_copy(w_uv_ref, w_uv, w_sem)
    w_copy.start()

    q32[...] = q_ref[...].astype(jnp.float32)
    cache[LAT + ROPE :, :] = jnp.zeros((cache.shape[0] - LAT - ROPE, cache.shape[1]), jnp.bfloat16)
    lane = lax.broadcasted_iota(jnp.int32, (requests, LANES), 1)
    for h in range(heads):
        at = slice(h * requests, (h + 1) * requests)
        nope = q32[pl.ds(h, requests, stride=ROWS), :].astype(jnp.bfloat16)
        latent = jnp.dot(nope, w_uk_ref[h], preferred_element_type=jnp.float32)
        rope = q32[pl.ds(heads + h % half, requests, stride=ROWS), :]
        if h >= half:
            rope = pltpu.roll(rope, LANES - ROPE, 1)
        query[at, :LAT] = latent.astype(jnp.bfloat16)
        query[at, LAT:] = jnp.where(lane < ROPE, rope, 0.0).astype(jnp.bfloat16)

    peak = mass = total = None

    def take(at, scores):
        nonlocal peak, mass, total
        highest = jnp.max(scores, axis=1, keepdims=True)
        if peak is not None:
            highest = jnp.maximum(peak, highest)
        weights = jnp.exp2(scores - highest)
        part = sum(weights[:, k : k + LANES] for k in range(0, width, LANES))
        values = lax.dot_general(
            weights.astype(jnp.bfloat16),
            cache[:LAT, at],
            (((1,), (1,)), ((), ())),
            preferred_element_type=jnp.float32,
        )
        if peak is None:
            mass, total = part, values
        else:
            keep = jnp.exp2(peak - highest)
            mass, total = mass * keep + part, total * keep + values
        peak = highest

    waiting = None
    for j in range(sum(pieces)):
        if j in firsts:
            piece(firsts.index(j)).wait()
            if j == firsts[-1]:
                w_copy.wait()
        at = slice(j * width, (j + 1) * width)
        scores = jnp.dot(query[...], cache[:, at], preferred_element_type=jnp.float32)
        hidden = jnp.where(pos_ref[:, at] < len_ref[...], 0.0, NEG)
        scores = scores.reshape(heads, requests, width) * SCALE + hidden[None]
        if waiting is not None:
            take(*waiting)
        waiting = (at, scores.reshape(rows, width))
    take(*waiting)
    mass = jnp.sum(mass, axis=1, keepdims=True)

    high = total.astype(jnp.bfloat16)
    low = (total - high.astype(jnp.float32)).astype(jnp.bfloat16)
    peaks = jnp.zeros((requests, LANES), jnp.float32)
    masses = jnp.zeros((requests, LANES), jnp.float32)
    packed[...] = jnp.zeros(packed.shape, jnp.float32)
    for h in range(heads):
        at = slice(h * requests, (h + 1) * requests)
        both = jnp.concatenate([high[at], low[at]], axis=0)
        value = jnp.dot(both, w_uv[h], preferred_element_type=jnp.float32)
        packed[pl.ds(h, requests, stride=ROWS), :] = value[:requests] + value[requests:]
        peaks = jnp.where(lane == h, peak[at], peaks)
        masses = jnp.where(lane == h, mass[at], masses)

    def terms(x, count):
        found = []
        for _ in range(count):
            term = x.astype(jnp.bfloat16).astype(jnp.float32)
            found.append(term)
            x = x - term
        return found

    stats = None
    for k, term in enumerate(terms(peaks, 3) + terms(masses, 2)):
        term = pltpu.roll(term, 16 * k, 1) if k else term
        stats = term if stats is None else stats + term
    packed[pl.ds(heads, requests, stride=ROWS), :] = stats
    out_ref[...] = packed[...].astype(jnp.bfloat16)


def segment(q, w_uk, positions, lens, cache_t, w_uv, pieces=(2, 6)):
    heads = w_uk.shape[0]
    requests = lens.shape[0]
    vmem = pl.BlockSpec(memory_space=pltpu.VMEM)
    hbm = pl.BlockSpec(memory_space=pltpu.HBM)
    return pl.pallas_call(
        functools.partial(segment_kernel, pieces=pieces),
        out_shape=jax.ShapeDtypeStruct((requests * ROWS, LANES), jnp.bfloat16),
        in_specs=[vmem, vmem, vmem, vmem, hbm, hbm],
        out_specs=vmem,
        scratch_shapes=[
            pltpu.VMEM((requests * ROWS, LANES), jnp.float32),
            pltpu.VMEM((heads * requests, LAT + LANES), jnp.bfloat16),
            pltpu.VMEM((LAT + LANES, cache_t.shape[1]), jnp.bfloat16),
            pltpu.VMEM(w_uv.shape, jnp.bfloat16),
            pltpu.VMEM((requests * ROWS, LANES), jnp.float32),
            pltpu.SemaphoreType.DMA((len(pieces),)),
            pltpu.SemaphoreType.DMA,
        ],
        compiler_params=pltpu.CompilerParams(vmem_limit_bytes=50 * 1024 * 1024),
        name="segment",
    )(q, w_uk, positions, lens, cache_t, w_uv)


def start_fetch(pairs, sems):
    copies = [pltpu.make_async_copy(a, b, sems.at[k]) for k, (a, b) in enumerate(pairs)]
    for copy in copies:
        copy.start()
    return copies


def fetch(pairs, sems):
    for copy in start_fetch(pairs, sems):
        copy.wait()


def pack_kernel(q_nope_hbm, q_rope_hbm, out_ref, q_nope_ref, q_rope_ref, sems):
    fetch([(q_nope_hbm, q_nope_ref), (q_rope_hbm, q_rope_ref)], sems)
    rope = q_rope_ref[...].astype(jnp.float32)
    half = rope.shape[0] // 2
    pairs = jnp.concatenate([rope[:half], rope[half:]], axis=1)
    block = jnp.concatenate([q_nope_ref[...].astype(jnp.float32), pairs], axis=0)
    block = block.astype(jnp.bfloat16)
    out_ref[...] = jnp.broadcast_to(block[None], out_ref.shape)


def pack(q_nope, q_rope, count):
    return pl.pallas_call(
        pack_kernel,
        out_shape=jax.ShapeDtypeStruct((count, ROWS, LANES), jnp.bfloat16),
        in_specs=[pl.BlockSpec(memory_space=pltpu.HBM)] * 2,
        out_specs=pl.BlockSpec(memory_space=pltpu.VMEM),
        scratch_shapes=[
            pltpu.VMEM(q_nope.shape, q_nope.dtype),
            pltpu.VMEM(q_rope.shape, q_rope.dtype),
            pltpu.SemaphoreType.DMA((2,)),
        ],
        compiler_params=pltpu.CompilerParams(vmem_limit_bytes=WHOLE_VMEM),
        name="pack",
    )(q_nope, q_rope)


def tail_kernel(
    q_nope_hbm,
    q_rope_hbm,
    w_uk_hbm,
    w_uv_hbm,
    suffix_hbm,
    len_ref,
    out_ref,
    stats_ref,
    q_nope_ref,
    q_rope_ref,
    w_uk_ref,
    suffix_ref,
    w_uv,
    sems,
):
    copies = start_fetch(
        [
            (q_nope_hbm, q_nope_ref),
            (q_rope_hbm, q_rope_ref),
            (w_uk_hbm, w_uk_ref),
            (suffix_hbm, suffix_ref),
            (w_uv_hbm, w_uv),
        ],
        sems,
    )
    for copy in copies[:-1]:
        copy.wait()
    heads = q_nope_ref.shape[0]

    def spread_heads(x):
        row = lax.broadcasted_iota(jnp.int32, x.shape, 0) % heads
        return jnp.concatenate(
            [jnp.where(row == h, x, 0.0).astype(jnp.bfloat16) for h in range(heads)], axis=1
        )

    latent = jnp.dot(
        spread_heads(q_nope_ref[...].astype(jnp.float32)),
        w_uk_ref[...].reshape(-1, LAT),
        preferred_element_type=jnp.float32,
    ).astype(jnp.bfloat16)
    scores = jnp.dot(latent, suffix_ref[:LAT, :], preferred_element_type=jnp.float32)
    scores = scores + jnp.dot(
        q_rope_ref[...], suffix_ref[LAT:, :], preferred_element_type=jnp.float32
    )
    slot = lax.broadcasted_iota(jnp.int32, scores.shape, 1)
    scores = scores * SCALE + jnp.where(slot < len_ref[0], 0.0, NEG)
    peak = jnp.max(scores, axis=1, keepdims=True)
    weights = jnp.exp2(scores - peak)
    mass = jnp.sum(weights, axis=1, keepdims=True)
    weighted = lax.dot_general(
        weights.astype(jnp.bfloat16),
        suffix_ref[:LAT, :],
        (((1,), (1,)), ((), ())),
        preferred_element_type=jnp.float32,
    )
    high = weighted.astype(jnp.bfloat16).astype(jnp.float32)
    both = spread_heads(jnp.concatenate([high, weighted - high], axis=0))
    copies[-1].wait()
    value = jnp.dot(both, w_uv[...].reshape(-1, LANES), preferred_element_type=jnp.float32)
    out_ref[...] = value[:heads] + value[heads:]
    row = lax.broadcasted_iota(jnp.int32, (heads, LANES), 0)
    lane = lax.broadcasted_iota(jnp.int32, (heads, LANES), 1)
    stats_ref[0:1, :] = jnp.sum(jnp.where(row == lane, peak, 0.0), axis=0, keepdims=True)
    stats_ref[1:2, :] = jnp.sum(jnp.where(row == lane, mass, 0.0), axis=0, keepdims=True)


def tail_part(q_nope, q_rope, w_uk, w_uv, suffix_t, suffix_len):
    vmem = pl.BlockSpec(memory_space=pltpu.VMEM)
    return pl.pallas_call(
        tail_kernel,
        out_shape=(
            jax.ShapeDtypeStruct((q_nope.shape[0], LANES), jnp.float32),
            jax.ShapeDtypeStruct((2, LANES), jnp.float32),
        ),
        in_specs=[pl.BlockSpec(memory_space=pltpu.HBM)] * 5
        + [pl.BlockSpec(memory_space=pltpu.SMEM)],
        out_specs=(vmem, vmem),
        scratch_shapes=[
            pltpu.VMEM(x.shape, x.dtype) for x in (q_nope, q_rope, w_uk, suffix_t, w_uv)
        ]
        + [pltpu.SemaphoreType.DMA((5,))],
        compiler_params=pltpu.CompilerParams(vmem_limit_bytes=WHOLE_VMEM),
        name="tail",
    )(q_nope, q_rope, w_uk, w_uv, suffix_t, suffix_len)


def combine_kernel(got_ref, tail_ref, tail_stats_ref, out_ref, got32, *, heads, sources):
    got32[...] = got_ref[...].astype(jnp.float32)
    stats = got32[pl.ds(heads, sources, stride=ROWS), :]

    def part(first, count):
        terms = [pltpu.roll(stats, (LANES - 16 * k) % LANES, 1) if k else stats for k in range(first, first + count)]
        return sum(terms[1:], terms[0])

    peak = part(0, 3)
    mass = part(3, 2)
    tail_peak = tail_stats_ref[0:1, :]
    tail_mass = tail_stats_ref[1:2, :]
    highest = jnp.maximum(jnp.max(peak, axis=0, keepdims=True), tail_peak)
    factor = jnp.exp2(peak - highest)
    tail_factor = jnp.exp2(tail_peak - highest)
    total = jnp.sum(factor * mass, axis=0, keepdims=True) + tail_factor * tail_mass
    lane = lax.broadcasted_iota(jnp.int32, total.shape, 1)
    total = jnp.where(lane < heads, total, 1.0)
    share = jnp.concatenate(
        [
            factor / total,
            jnp.broadcast_to(tail_factor / total, (8, LANES)),
            jnp.zeros((LANES - sources - 8, LANES), jnp.float32),
        ],
        axis=0,
    )
    share = share.T[:heads]
    value = tail_ref[...] * share[:, sources : sources + 1]
    for s in range(sources):
        value = value + got32[s * ROWS : s * ROWS + heads, :] * share[:, s : s + 1]
    value = value.astype(jnp.bfloat16)
    for s in range(sources):
        out_ref[s * heads : (s + 1) * heads, :] = value


def combine(got, tail, tail_stats, sources):
    heads = tail.shape[0]
    return pl.pallas_call(
        functools.partial(combine_kernel, heads=heads, sources=sources),
        out_shape=jax.ShapeDtypeStruct((sources * heads, LANES), jnp.bfloat16),
        in_specs=[pl.BlockSpec(memory_space=pltpu.VMEM)] * 3,
        out_specs=pl.BlockSpec(memory_space=pltpu.VMEM),
        scratch_shapes=[pltpu.VMEM((sources * ROWS, LANES), jnp.float32)],
        compiler_params=pltpu.CompilerParams(vmem_limit_bytes=8 * 1024 * 1024),
        name="combine",
    )(got, tail, tail_stats)


def output_kernel(values_ref, w_ref, out_ref, values32, flat, *, heads, requests, first):
    values32[...] = values_ref[...].astype(jnp.float32)
    for h in range(heads):
        value = values32[pl.ds(h, requests, stride=heads), :]
        flat[:, h * LANES : (h + 1) * LANES] = pltpu.roll(value, CTX_FIRST, 0).astype(jnp.bfloat16)
    product = lax.dot_general(
        flat[...], w_ref[...], (((1,), (1,)), ((), ())), preferred_element_type=jnp.float32
    )
    out_ref[: requests - first, :] = product[first:]
    out_ref[requests - first :, :] = product[:first]


def output_product(values, w_out_t, requests, first):
    heads = values.shape[0] // requests
    return pl.pallas_call(
        functools.partial(output_kernel, heads=heads, requests=requests, first=first),
        out_shape=jax.ShapeDtypeStruct((requests, w_out_t.shape[0]), jnp.float32),
        in_specs=[pl.BlockSpec(memory_space=pltpu.VMEM)] * 2,
        out_specs=pl.BlockSpec(memory_space=pltpu.VMEM),
        scratch_shapes=[
            pltpu.VMEM(values.shape, jnp.float32),
            pltpu.VMEM((requests, heads * LANES), jnp.bfloat16),
        ],
        compiler_params=pltpu.CompilerParams(vmem_limit_bytes=8 * 1024 * 1024),
        name="output_product",
    )(values, w_out_t)


def exchange(value, axis, first):
    count = lax.axis_size(axis)
    order = [[(k + first) % count for k in range(count)]]
    return lax.all_to_all(value, axis, 0, 0, axis_index_groups=order, tiled=True)


def on_device(
    q_nope,
    q_rope,
    w_uk,
    w_uv,
    w_out,
    prefix_cache,
    block_table,
    prefix_len,
    suffix_cache,
    suffix_len,
):
    requests = prefix_len.shape[0]
    heads = w_uk.shape[0]
    raw = exchange(pack(q_nope[0], q_rope[0], requests), "ctx", CTX_FIRST)
    tail, tail_stats = tail_part(
        q_nope[0], q_rope[0], w_uk, w_uv, suffix_cache[0].T, suffix_len
    )
    positions = (
        block_table[:, None] * BLOCK + jnp.arange(BLOCK, dtype=jnp.int32)[None, :]
    ).reshape(1, -1)
    raw, tail, tail_stats = lax.optimization_barrier((raw, tail, tail_stats))
    packed = segment(
        raw.reshape(requests * ROWS, LANES),
        w_uk,
        positions,
        jnp.roll(prefix_len, -CTX_FIRST)[:, None],
        prefix_cache.T,
        w_uv,
    )
    got = exchange(packed.reshape(requests, ROWS, LANES), "ctx", CTX_FIRST)
    values = combine(got.reshape(requests * ROWS, LANES), tail, tail_stats, requests)
    every = exchange(values.reshape(requests, heads, LANES), "ctx", CTX_FIRST)
    tp = lax.axis_size("tp")
    first = TP_FIRST * (requests // tp)
    partial = output_product(every.reshape(requests * heads, LANES), w_out.T, requests, first)
    pieces = exchange(partial.reshape(tp, requests // tp, -1), "tp", TP_FIRST)
    return pieces.sum(axis=0).astype(jnp.bfloat16)


def solution(mesh):
    placed = (
        P("ctx", "tp", None),
        P("ctx", "tp", None),
        P("tp", None, None),
        P("tp", None, None),
        P("tp", "ctx"),
        P("ctx", None),
        P("ctx"),
        P(),
        P("ctx", None, None),
        P("ctx"),
    )
    return jax.shard_map(
        on_device, mesh=mesh, in_specs=placed, out_specs=P("tp", "ctx"), check_vma=False
    )
```

```python
import functools
import math

import jax
import jax.numpy as jnp
from jax import lax
from jax.experimental import pallas as pl
from jax.experimental.pallas import tpu as pltpu
from jax.sharding import PartitionSpec as P

LAT = 512
ROPE = 64
NOPE = 128
BLOCK = 64
LANES = 128
ROWS = 24
NEG = -1e30
CTX_FIRST = 18
TP_FIRST = 4
WHOLE_VMEM = 60 * 1024 * 1024
SCALE = (NOPE + ROPE) ** -0.5 * math.log2(math.e)


def segment_kernel(
    q_ref,
    w_uk_ref,
    pos_ref,
    len_ref,
    cache_ref,
    w_uv_ref,
    out_ref,
    q32,
    query,
    cache,
    w_uv,
    packed,
    cache_sems,
    w_sem,
    *,
    pieces,
):
    requests = len_ref.shape[0]
    heads = w_uk_ref.shape[0]
    half = heads // 2
    rows = heads * requests
    width = cache.shape[1] // sum(pieces)
    firsts = [sum(pieces[:k]) for k in range(len(pieces))]

    def piece(k):
        at = pl.ds(firsts[k] * width, pieces[k] * width)
        return pltpu.make_async_copy(
            cache_ref.at[:, at], cache.at[pl.ds(0, LAT + ROPE), at], cache_sems.at[k]
        )

    for k in range(len(pieces)):
        piece(k).start()
    w_copy = pltpu.make_async_copy(w_uv_ref, w_uv, w_sem)
    w_copy.start()

    q32[...] = q_ref[...].astype(jnp.float32)
    cache[LAT + ROPE :, :] = jnp.zeros((cache.shape[0] - LAT - ROPE, cache.shape[1]), jnp.bfloat16)
    lane = lax.broadcasted_iota(jnp.int32, (requests, LANES), 1)
    for h in range(heads):
        at = slice(h * requests, (h + 1) * requests)
        nope = q32[pl.ds(h, requests, stride=ROWS), :].astype(jnp.bfloat16)
        latent = jnp.dot(nope, w_uk_ref[h], preferred_element_type=jnp.float32)
        rope = q32[pl.ds(heads + h % half, requests, stride=ROWS), :]
        if h >= half:
            rope = pltpu.roll(rope, LANES - ROPE, 1)
        query[at, :LAT] = latent.astype(jnp.bfloat16)
        query[at, LAT:] = jnp.where(lane < ROPE, rope, 0.0).astype(jnp.bfloat16)

    peak = mass = total = None

    def take(at, scores):
        nonlocal peak, mass, total
        highest = jnp.max(scores, axis=1, keepdims=True)
        if peak is not None:
            highest = jnp.maximum(peak, highest)
        weights = jnp.exp2(scores - highest)
        part = sum(weights[:, k : k + LANES] for k in range(0, width, LANES))
        values = lax.dot_general(
            weights.astype(jnp.bfloat16),
            cache[:LAT, at],
            (((1,), (1,)), ((), ())),
            preferred_element_type=jnp.float32,
        )
        if peak is None:
            mass, total = part, values
        else:
            keep = jnp.exp2(peak - highest)
            mass, total = mass * keep + part, total * keep + values
        peak = highest

    waiting = None
    for j in range(sum(pieces)):
        if j in firsts:
            piece(firsts.index(j)).wait()
            if j == firsts[-1]:
                w_copy.wait()
        at = slice(j * width, (j + 1) * width)
        scores = jnp.dot(query[...], cache[:, at], preferred_element_type=jnp.float32)
        hidden = jnp.where(pos_ref[:, at] < len_ref[:, :1], 0.0, NEG)
        scores = scores.reshape(heads, requests, width) * SCALE + hidden[None]
        if waiting is not None:
            take(*waiting)
        waiting = (at, scores.reshape(rows, width))
    take(*waiting)
    mass = jnp.sum(mass, axis=1, keepdims=True)

    high = total.astype(jnp.bfloat16)
    low = (total - high.astype(jnp.float32)).astype(jnp.bfloat16)
    peaks = jnp.zeros((requests, LANES), jnp.float32)
    masses = jnp.zeros((requests, LANES), jnp.float32)
    packed[...] = jnp.zeros(packed.shape, jnp.float32)
    for h in range(heads):
        at = slice(h * requests, (h + 1) * requests)
        both = jnp.concatenate([high[at], low[at]], axis=0)
        value = jnp.dot(both, w_uv[h], preferred_element_type=jnp.float32)
        packed[pl.ds(h, requests, stride=ROWS), :] = value[:requests] + value[requests:]
        peaks = jnp.where(lane == h, peak[at], peaks)
        masses = jnp.where(lane == h, mass[at], masses)

    def terms(x, count):
        found = []
        for _ in range(count):
            term = x.astype(jnp.bfloat16).astype(jnp.float32)
            found.append(term)
            x = x - term
        return found

    stats = None
    for k, term in enumerate(terms(peaks, 3) + terms(masses, 2)):
        term = pltpu.roll(term, 16 * k, 1) if k else term
        stats = term if stats is None else stats + term
    packed[pl.ds(heads, requests, stride=ROWS), :] = stats
    out_ref[...] = packed[...].astype(jnp.bfloat16)


def segment(q, w_uk, positions, lens, cache_t, w_uv, pieces=(2, 6)):
    heads = w_uk.shape[0]
    requests = lens.shape[0]
    vmem = pl.BlockSpec(memory_space=pltpu.VMEM)
    hbm = pl.BlockSpec(memory_space=pltpu.HBM)
    return pl.pallas_call(
        functools.partial(segment_kernel, pieces=pieces),
        out_shape=jax.ShapeDtypeStruct((requests * ROWS, LANES), jnp.bfloat16),
        in_specs=[vmem, vmem, vmem, vmem, hbm, hbm],
        out_specs=vmem,
        scratch_shapes=[
            pltpu.VMEM((requests * ROWS, LANES), jnp.float32),
            pltpu.VMEM((heads * requests, LAT + LANES), jnp.bfloat16),
            pltpu.VMEM((LAT + LANES, cache_t.shape[1]), jnp.bfloat16),
            pltpu.VMEM(w_uv.shape, jnp.bfloat16),
            pltpu.VMEM((requests * ROWS, LANES), jnp.float32),
            pltpu.SemaphoreType.DMA((len(pieces),)),
            pltpu.SemaphoreType.DMA,
        ],
        compiler_params=pltpu.CompilerParams(vmem_limit_bytes=50 * 1024 * 1024),
        name="segment",
    )(q, w_uk, positions, lens, cache_t, w_uv)


def start_fetch(pairs, sems):
    copies = [pltpu.make_async_copy(a, b, sems.at[k]) for k, (a, b) in enumerate(pairs)]
    for copy in copies:
        copy.start()
    return copies


def fetch(pairs, sems):
    for copy in start_fetch(pairs, sems):
        copy.wait()


def pack_kernel(
    q_nope_hbm,
    q_rope_hbm,
    table_hbm,
    lens_hbm,
    out_ref,
    pos_ref,
    len_ref,
    q_nope_ref,
    q_rope_ref,
    table,
    lens,
    sems,
):
    fetch(
        [
            (q_nope_hbm, q_nope_ref),
            (q_rope_hbm, q_rope_ref),
            (table_hbm, table),
            (lens_hbm, lens),
        ],
        sems,
    )
    rope = q_rope_ref[...].astype(jnp.float32)
    half = rope.shape[0] // 2
    pairs = jnp.concatenate([rope[:half], rope[half:]], axis=1)
    block = jnp.concatenate([q_nope_ref[...].astype(jnp.float32), pairs], axis=0)
    block = block.astype(jnp.bfloat16)
    out_ref[...] = jnp.broadcast_to(block[None], out_ref.shape)

    lane = lax.broadcasted_iota(jnp.int32, (1, LANES), 1)
    for k in range(0, table.shape[0], LANES // BLOCK):
        start = jnp.where(lane < BLOCK, table[k], table[k + 1])
        pos_ref[:, k * BLOCK : k * BLOCK + LANES] = start * BLOCK + lane % BLOCK
    count = lens.shape[0]
    row = lax.broadcasted_iota(jnp.int32, (count, LANES), 0)
    limit = jnp.zeros((count, LANES), jnp.int32)
    for r in range(count):
        limit = jnp.where(row == r, lens[(r + CTX_FIRST) % count], limit)
    len_ref[...] = limit


def pack(q_nope, q_rope, table, lens):
    count = lens.shape[0]
    return pl.pallas_call(
        pack_kernel,
        out_shape=(
            jax.ShapeDtypeStruct((count, ROWS, LANES), jnp.bfloat16),
            jax.ShapeDtypeStruct((1, table.shape[0] * BLOCK), jnp.int32),
            jax.ShapeDtypeStruct((count, LANES), jnp.int32),
        ),
        in_specs=[pl.BlockSpec(memory_space=pltpu.HBM)] * 4,
        out_specs=(pl.BlockSpec(memory_space=pltpu.VMEM),) * 3,
        scratch_shapes=[
            pltpu.VMEM(q_nope.shape, q_nope.dtype),
            pltpu.VMEM(q_rope.shape, q_rope.dtype),
            pltpu.SMEM(table.shape, table.dtype),
            pltpu.SMEM(lens.shape, lens.dtype),
            pltpu.SemaphoreType.DMA((4,)),
        ],
        compiler_params=pltpu.CompilerParams(vmem_limit_bytes=WHOLE_VMEM),
        name="pack",
    )(q_nope, q_rope, table, lens)


def tail_kernel(
    q_nope_hbm,
    q_rope_hbm,
    w_uk_hbm,
    w_uv_hbm,
    suffix_hbm,
    len_ref,
    out_ref,
    stats_ref,
    q_nope_ref,
    q_rope_ref,
    w_uk_ref,
    suffix_ref,
    w_uv,
    sems,
):
    copies = start_fetch(
        [
            (q_nope_hbm, q_nope_ref),
            (q_rope_hbm, q_rope_ref),
            (w_uk_hbm, w_uk_ref),
            (suffix_hbm, suffix_ref),
            (w_uv_hbm, w_uv),
        ],
        sems,
    )
    for copy in copies[:-1]:
        copy.wait()
    heads = q_nope_ref.shape[0]

    def spread_heads(x):
        row = lax.broadcasted_iota(jnp.int32, x.shape, 0) % heads
        return jnp.concatenate(
            [jnp.where(row == h, x, 0.0).astype(jnp.bfloat16) for h in range(heads)], axis=1
        )

    latent = jnp.dot(
        spread_heads(q_nope_ref[...].astype(jnp.float32)),
        w_uk_ref[...].reshape(-1, LAT),
        preferred_element_type=jnp.float32,
    ).astype(jnp.bfloat16)
    scores = jnp.dot(latent, suffix_ref[:LAT, :], preferred_element_type=jnp.float32)
    scores = scores + jnp.dot(
        q_rope_ref[...], suffix_ref[LAT:, :], preferred_element_type=jnp.float32
    )
    slot = lax.broadcasted_iota(jnp.int32, scores.shape, 1)
    scores = scores * SCALE + jnp.where(slot < len_ref[0], 0.0, NEG)
    peak = jnp.max(scores, axis=1, keepdims=True)
    weights = jnp.exp2(scores - peak)
    mass = jnp.sum(weights, axis=1, keepdims=True)
    weighted = lax.dot_general(
        weights.astype(jnp.bfloat16),
        suffix_ref[:LAT, :],
        (((1,), (1,)), ((), ())),
        preferred_element_type=jnp.float32,
    )
    high = weighted.astype(jnp.bfloat16).astype(jnp.float32)
    both = spread_heads(jnp.concatenate([high, weighted - high], axis=0))
    copies[-1].wait()
    value = jnp.dot(both, w_uv[...].reshape(-1, LANES), preferred_element_type=jnp.float32)
    out_ref[...] = value[:heads] + value[heads:]
    row = lax.broadcasted_iota(jnp.int32, (heads, LANES), 0)
    lane = lax.broadcasted_iota(jnp.int32, (heads, LANES), 1)
    stats_ref[0:1, :] = jnp.sum(jnp.where(row == lane, peak, 0.0), axis=0, keepdims=True)
    stats_ref[1:2, :] = jnp.sum(jnp.where(row == lane, mass, 0.0), axis=0, keepdims=True)


def tail_part(q_nope, q_rope, w_uk, w_uv, suffix_t, suffix_len):
    vmem = pl.BlockSpec(memory_space=pltpu.VMEM)
    return pl.pallas_call(
        tail_kernel,
        out_shape=(
            jax.ShapeDtypeStruct((q_nope.shape[0], LANES), jnp.float32),
            jax.ShapeDtypeStruct((2, LANES), jnp.float32),
        ),
        in_specs=[pl.BlockSpec(memory_space=pltpu.HBM)] * 5
        + [pl.BlockSpec(memory_space=pltpu.SMEM)],
        out_specs=(vmem, vmem),
        scratch_shapes=[
            pltpu.VMEM(x.shape, x.dtype) for x in (q_nope, q_rope, w_uk, suffix_t, w_uv)
        ]
        + [pltpu.SemaphoreType.DMA((5,))],
        compiler_params=pltpu.CompilerParams(vmem_limit_bytes=WHOLE_VMEM),
        name="tail",
    )(q_nope, q_rope, w_uk, w_uv, suffix_t, suffix_len)


def combine_kernel(got_ref, tail_ref, tail_stats_ref, out_ref, got32, *, heads, sources):
    got32[...] = got_ref[...].astype(jnp.float32)
    stats = got32[pl.ds(heads, sources, stride=ROWS), :]

    def part(first, count):
        terms = [pltpu.roll(stats, (LANES - 16 * k) % LANES, 1) if k else stats for k in range(first, first + count)]
        return sum(terms[1:], terms[0])

    peak = part(0, 3)
    mass = part(3, 2)
    tail_peak = tail_stats_ref[0:1, :]
    tail_mass = tail_stats_ref[1:2, :]
    highest = jnp.maximum(jnp.max(peak, axis=0, keepdims=True), tail_peak)
    factor = jnp.exp2(peak - highest)
    tail_factor = jnp.exp2(tail_peak - highest)
    total = jnp.sum(factor * mass, axis=0, keepdims=True) + tail_factor * tail_mass
    lane = lax.broadcasted_iota(jnp.int32, total.shape, 1)
    total = jnp.where(lane < heads, total, 1.0)
    share = jnp.concatenate(
        [
            factor / total,
            jnp.broadcast_to(tail_factor / total, (8, LANES)),
            jnp.zeros((LANES - sources - 8, LANES), jnp.float32),
        ],
        axis=0,
    )
    share = share.T[:heads]
    value = tail_ref[...] * share[:, sources : sources + 1]
    for s in range(sources):
        value = value + got32[s * ROWS : s * ROWS + heads, :] * share[:, s : s + 1]
    value = value.astype(jnp.bfloat16)
    for s in range(sources):
        out_ref[s * heads : (s + 1) * heads, :] = value


def combine(got, tail, tail_stats, sources):
    heads = tail.shape[0]
    return pl.pallas_call(
        functools.partial(combine_kernel, heads=heads, sources=sources),
        out_shape=jax.ShapeDtypeStruct((sources * heads, LANES), jnp.bfloat16),
        in_specs=[pl.BlockSpec(memory_space=pltpu.VMEM)] * 3,
        out_specs=pl.BlockSpec(memory_space=pltpu.VMEM),
        scratch_shapes=[pltpu.VMEM((sources * ROWS, LANES), jnp.float32)],
        compiler_params=pltpu.CompilerParams(vmem_limit_bytes=8 * 1024 * 1024),
        name="combine",
    )(got, tail, tail_stats)


def output_kernel(values_ref, w_ref, out_ref, values32, flat, *, heads, requests, first):
    values32[...] = values_ref[...].astype(jnp.float32)
    for h in range(heads):
        value = values32[pl.ds(h, requests, stride=heads), :]
        flat[:, h * LANES : (h + 1) * LANES] = pltpu.roll(value, CTX_FIRST, 0).astype(jnp.bfloat16)
    product = lax.dot_general(
        flat[...], w_ref[...], (((1,), (1,)), ((), ())), preferred_element_type=jnp.float32
    )
    out_ref[: requests - first, :] = product[first:]
    out_ref[requests - first :, :] = product[:first]


def output_product(values, w_out_t, requests, first):
    heads = values.shape[0] // requests
    return pl.pallas_call(
        functools.partial(output_kernel, heads=heads, requests=requests, first=first),
        out_shape=jax.ShapeDtypeStruct((requests, w_out_t.shape[0]), jnp.float32),
        in_specs=[pl.BlockSpec(memory_space=pltpu.VMEM)] * 2,
        out_specs=pl.BlockSpec(memory_space=pltpu.VMEM),
        scratch_shapes=[
            pltpu.VMEM(values.shape, jnp.float32),
            pltpu.VMEM((requests, heads * LANES), jnp.bfloat16),
        ],
        compiler_params=pltpu.CompilerParams(vmem_limit_bytes=8 * 1024 * 1024),
        name="output_product",
    )(values, w_out_t)


def exchange(value, axis, first):
    count = lax.axis_size(axis)
    order = [[(k + first) % count for k in range(count)]]
    return lax.all_to_all(value, axis, 0, 0, axis_index_groups=order, tiled=True)


def on_device(
    q_nope,
    q_rope,
    w_uk,
    w_uv,
    w_out,
    prefix_cache,
    block_table,
    prefix_len,
    suffix_cache,
    suffix_len,
):
    requests = prefix_len.shape[0]
    heads = w_uk.shape[0]
    packed_query, positions, lens = pack(q_nope[0], q_rope[0], block_table, prefix_len)
    raw = exchange(packed_query, "ctx", CTX_FIRST)
    tail, tail_stats = tail_part(
        q_nope[0], q_rope[0], w_uk, w_uv, suffix_cache[0].T, suffix_len
    )
    raw, tail, tail_stats = lax.optimization_barrier((raw, tail, tail_stats))
    packed = segment(
        raw.reshape(requests * ROWS, LANES),
        w_uk,
        positions,
        lens,
        prefix_cache.T,
        w_uv,
    )
    got = exchange(packed.reshape(requests, ROWS, LANES), "ctx", CTX_FIRST)
    values = combine(got.reshape(requests * ROWS, LANES), tail, tail_stats, requests)
    every = exchange(values.reshape(requests, heads, LANES), "ctx", CTX_FIRST)
    tp = lax.axis_size("tp")
    first = TP_FIRST * (requests // tp)
    partial = output_product(every.reshape(requests * heads, LANES), w_out.T, requests, first)
    pieces = exchange(partial.reshape(tp, requests // tp, -1), "tp", TP_FIRST)
    return pieces.sum(axis=0).astype(jnp.bfloat16)


def solution(mesh):
    placed = (
        P("ctx", "tp", None),
        P("ctx", "tp", None),
        P("tp", None, None),
        P("tp", None, None),
        P("tp", "ctx"),
        P("ctx", None),
        P("ctx"),
        P(),
        P("ctx", None, None),
        P("ctx"),
    )
    return jax.shard_map(
        on_device, mesh=mesh, in_specs=placed, out_specs=P("tp", "ctx"), check_vma=False
    )
```

```python
import functools
import math

import jax
import jax.numpy as jnp
from jax import lax
from jax.experimental import pallas as pl
from jax.experimental.pallas import tpu as pltpu
from jax.sharding import PartitionSpec as P

LAT = 512
ROPE = 64
NOPE = 128
BLOCK = 64
LANES = 128
ROWS = 24
NEG = -1e30
CTX_FIRST = 18
TP_FIRST = 4
WHOLE_VMEM = 60 * 1024 * 1024
SCALE = (NOPE + ROPE) ** -0.5 * math.log2(math.e)


def segment_kernel(
    q_ref,
    w_uk_ref,
    pos_ref,
    len_ref,
    cache_ref,
    w_uv_ref,
    out_ref,
    q32,
    query,
    cache,
    w_uv,
    packed,
    cache_sems,
    w_sem,
    *,
    pieces,
):
    requests = len_ref.shape[0]
    heads = w_uk_ref.shape[0]
    half = heads // 2
    rows = heads * requests
    width = cache.shape[1] // sum(pieces)
    firsts = [sum(pieces[:k]) for k in range(len(pieces))]

    def piece(k):
        at = pl.ds(firsts[k] * width, pieces[k] * width)
        return pltpu.make_async_copy(
            cache_ref.at[:, at], cache.at[:, at], cache_sems.at[k]
        )

    for k in range(len(pieces)):
        piece(k).start()
    w_copy = pltpu.make_async_copy(w_uv_ref, w_uv, w_sem)
    w_copy.start()

    q32[...] = q_ref[...].astype(jnp.float32)
    lane = lax.broadcasted_iota(jnp.int32, (requests, LANES), 1)
    for h in range(heads):
        at = slice(h * requests, (h + 1) * requests)
        nope = q32[pl.ds(h, requests, stride=ROWS), :].astype(jnp.bfloat16)
        latent = jnp.dot(nope, w_uk_ref[h], preferred_element_type=jnp.float32)
        rope = q32[pl.ds(heads + h % half, requests, stride=ROWS), :]
        if h >= half:
            rope = pltpu.roll(rope, LANES - ROPE, 1)
        query[at, :LAT] = latent.astype(jnp.bfloat16)
        query[at, LAT:] = rope[:, :ROPE].astype(jnp.bfloat16)

    peak = mass = total = None

    def take(at, scores):
        nonlocal peak, mass, total
        highest = jnp.max(scores, axis=1, keepdims=True)
        if peak is not None:
            highest = jnp.maximum(peak, highest)
        weights = jnp.exp2(scores - highest)
        part = sum(weights[:, k : k + LANES] for k in range(0, width, LANES))
        values = lax.dot_general(
            weights.astype(jnp.bfloat16),
            cache[:LAT, at],
            (((1,), (1,)), ((), ())),
            preferred_element_type=jnp.float32,
        )
        if peak is None:
            mass, total = part, values
        else:
            keep = jnp.exp2(peak - highest)
            mass, total = mass * keep + part, total * keep + values
        peak = highest

    waiting = None
    for j in range(sum(pieces)):
        if j in firsts:
            piece(firsts.index(j)).wait()
            if j == firsts[-1]:
                w_copy.wait()
        at = slice(j * width, (j + 1) * width)
        scores = jnp.dot(query[...], cache[:, at], preferred_element_type=jnp.float32)
        hidden = jnp.where(pos_ref[:, at] < len_ref[:, :1], 0.0, NEG)
        scores = scores.reshape(heads, requests, width) * SCALE + hidden[None]
        if waiting is not None:
            take(*waiting)
        waiting = (at, scores.reshape(rows, width))
    take(*waiting)
    mass = jnp.sum(mass, axis=1, keepdims=True)

    high = total.astype(jnp.bfloat16)
    low = (total - high.astype(jnp.float32)).astype(jnp.bfloat16)
    peaks = jnp.zeros((requests, LANES), jnp.float32)
    masses = jnp.zeros((requests, LANES), jnp.float32)
    packed[...] = jnp.zeros(packed.shape, jnp.float32)
    for h in range(heads):
        at = slice(h * requests, (h + 1) * requests)
        both = jnp.concatenate([high[at], low[at]], axis=0)
        value = jnp.dot(both, w_uv[h], preferred_element_type=jnp.float32)
        packed[pl.ds(h, requests, stride=ROWS), :] = value[:requests] + value[requests:]
        peaks = jnp.where(lane == h, peak[at], peaks)
        masses = jnp.where(lane == h, mass[at], masses)

    def terms(x, count):
        found = []
        for _ in range(count):
            term = x.astype(jnp.bfloat16).astype(jnp.float32)
            found.append(term)
            x = x - term
        return found

    stats = None
    for k, term in enumerate(terms(peaks, 3) + terms(masses, 2)):
        term = pltpu.roll(term, 16 * k, 1) if k else term
        stats = term if stats is None else stats + term
    packed[pl.ds(heads, requests, stride=ROWS), :] = stats
    out_ref[...] = packed[...].astype(jnp.bfloat16)


def segment(q, w_uk, positions, lens, cache_t, w_uv, pieces=(2, 6)):
    heads = w_uk.shape[0]
    requests = lens.shape[0]
    vmem = pl.BlockSpec(memory_space=pltpu.VMEM)
    hbm = pl.BlockSpec(memory_space=pltpu.HBM)
    return pl.pallas_call(
        functools.partial(segment_kernel, pieces=pieces),
        out_shape=jax.ShapeDtypeStruct((requests * ROWS, LANES), jnp.bfloat16),
        in_specs=[vmem, vmem, vmem, vmem, hbm, hbm],
        out_specs=vmem,
        scratch_shapes=[
            pltpu.VMEM((requests * ROWS, LANES), jnp.float32),
            pltpu.VMEM((heads * requests, LAT + ROPE), jnp.bfloat16),
            pltpu.VMEM(cache_t.shape, jnp.bfloat16),
            pltpu.VMEM(w_uv.shape, jnp.bfloat16),
            pltpu.VMEM((requests * ROWS, LANES), jnp.float32),
            pltpu.SemaphoreType.DMA((len(pieces),)),
            pltpu.SemaphoreType.DMA,
        ],
        compiler_params=pltpu.CompilerParams(vmem_limit_bytes=50 * 1024 * 1024),
        name="segment",
    )(q, w_uk, positions, lens, cache_t, w_uv)


def start_fetch(pairs, sems):
    copies = [pltpu.make_async_copy(a, b, sems.at[k]) for k, (a, b) in enumerate(pairs)]
    for copy in copies:
        copy.start()
    return copies


def fetch(pairs, sems):
    for copy in start_fetch(pairs, sems):
        copy.wait()


def pack_kernel(
    q_nope_hbm,
    q_rope_hbm,
    table_hbm,
    lens_hbm,
    out_ref,
    pos_ref,
    len_ref,
    q_nope_ref,
    q_rope_ref,
    table,
    lens,
    sems,
):
    fetch(
        [
            (q_nope_hbm, q_nope_ref),
            (q_rope_hbm, q_rope_ref),
            (table_hbm, table),
            (lens_hbm, lens),
        ],
        sems,
    )
    rope = q_rope_ref[...].astype(jnp.float32)
    half = rope.shape[0] // 2
    pairs = jnp.concatenate([rope[:half], rope[half:]], axis=1)
    block = jnp.concatenate([q_nope_ref[...].astype(jnp.float32), pairs], axis=0)
    block = block.astype(jnp.bfloat16)
    out_ref[...] = jnp.broadcast_to(block[None], out_ref.shape)

    lane = lax.broadcasted_iota(jnp.int32, (1, LANES), 1)
    for k in range(0, table.shape[0], LANES // BLOCK):
        start = jnp.where(lane < BLOCK, table[k], table[k + 1])
        pos_ref[:, k * BLOCK : k * BLOCK + LANES] = start * BLOCK + lane % BLOCK
    count = lens.shape[0]
    row = lax.broadcasted_iota(jnp.int32, (count, LANES), 0)
    limit = jnp.zeros((count, LANES), jnp.int32)
    for r in range(count):
        limit = jnp.where(row == r, lens[(r + CTX_FIRST) % count], limit)
    len_ref[...] = limit


def pack(q_nope, q_rope, table, lens):
    count = lens.shape[0]
    return pl.pallas_call(
        pack_kernel,
        out_shape=(
            jax.ShapeDtypeStruct((count, ROWS, LANES), jnp.bfloat16),
            jax.ShapeDtypeStruct((1, table.shape[0] * BLOCK), jnp.int32),
            jax.ShapeDtypeStruct((count, LANES), jnp.int32),
        ),
        in_specs=[pl.BlockSpec(memory_space=pltpu.HBM)] * 4,
        out_specs=(pl.BlockSpec(memory_space=pltpu.VMEM),) * 3,
        scratch_shapes=[
            pltpu.VMEM(q_nope.shape, q_nope.dtype),
            pltpu.VMEM(q_rope.shape, q_rope.dtype),
            pltpu.SMEM(table.shape, table.dtype),
            pltpu.SMEM(lens.shape, lens.dtype),
            pltpu.SemaphoreType.DMA((4,)),
        ],
        compiler_params=pltpu.CompilerParams(vmem_limit_bytes=WHOLE_VMEM),
        name="pack",
    )(q_nope, q_rope, table, lens)


def tail_kernel(
    q_nope_hbm,
    q_rope_hbm,
    w_uk_hbm,
    w_uv_hbm,
    suffix_hbm,
    len_ref,
    out_ref,
    stats_ref,
    q_nope_ref,
    q_rope_ref,
    w_uk_ref,
    suffix_ref,
    w_uv,
    sems,
):
    copies = start_fetch(
        [
            (q_nope_hbm, q_nope_ref),
            (q_rope_hbm, q_rope_ref),
            (w_uk_hbm, w_uk_ref),
            (suffix_hbm, suffix_ref),
            (w_uv_hbm, w_uv),
        ],
        sems,
    )
    for copy in copies[:-1]:
        copy.wait()
    heads = q_nope_ref.shape[0]

    def spread_heads(x):
        row = lax.broadcasted_iota(jnp.int32, x.shape, 0) % heads
        return jnp.concatenate(
            [jnp.where(row == h, x, 0.0).astype(jnp.bfloat16) for h in range(heads)], axis=1
        )

    latent = jnp.dot(
        spread_heads(q_nope_ref[...].astype(jnp.float32)),
        w_uk_ref[...].reshape(-1, LAT),
        preferred_element_type=jnp.float32,
    ).astype(jnp.bfloat16)
    scores = jnp.dot(latent, suffix_ref[:LAT, :], preferred_element_type=jnp.float32)
    scores = scores + jnp.dot(
        q_rope_ref[...], suffix_ref[LAT:, :], preferred_element_type=jnp.float32
    )
    slot = lax.broadcasted_iota(jnp.int32, scores.shape, 1)
    scores = scores * SCALE + jnp.where(slot < len_ref[0], 0.0, NEG)
    peak = jnp.max(scores, axis=1, keepdims=True)
    weights = jnp.exp2(scores - peak)
    mass = jnp.sum(weights, axis=1, keepdims=True)
    weighted = lax.dot_general(
        weights.astype(jnp.bfloat16),
        suffix_ref[:LAT, :],
        (((1,), (1,)), ((), ())),
        preferred_element_type=jnp.float32,
    )
    high = weighted.astype(jnp.bfloat16).astype(jnp.float32)
    both = spread_heads(jnp.concatenate([high, weighted - high], axis=0))
    copies[-1].wait()
    value = jnp.dot(both, w_uv[...].reshape(-1, LANES), preferred_element_type=jnp.float32)
    out_ref[...] = value[:heads] + value[heads:]
    row = lax.broadcasted_iota(jnp.int32, (heads, LANES), 0)
    lane = lax.broadcasted_iota(jnp.int32, (heads, LANES), 1)
    stats_ref[0:1, :] = jnp.sum(jnp.where(row == lane, peak, 0.0), axis=0, keepdims=True)
    stats_ref[1:2, :] = jnp.sum(jnp.where(row == lane, mass, 0.0), axis=0, keepdims=True)


def tail_part(q_nope, q_rope, w_uk, w_uv, suffix_t, suffix_len):
    vmem = pl.BlockSpec(memory_space=pltpu.VMEM)
    return pl.pallas_call(
        tail_kernel,
        out_shape=(
            jax.ShapeDtypeStruct((q_nope.shape[0], LANES), jnp.float32),
            jax.ShapeDtypeStruct((2, LANES), jnp.float32),
        ),
        in_specs=[pl.BlockSpec(memory_space=pltpu.HBM)] * 5
        + [pl.BlockSpec(memory_space=pltpu.SMEM)],
        out_specs=(vmem, vmem),
        scratch_shapes=[
            pltpu.VMEM(x.shape, x.dtype) for x in (q_nope, q_rope, w_uk, suffix_t, w_uv)
        ]
        + [pltpu.SemaphoreType.DMA((5,))],
        compiler_params=pltpu.CompilerParams(vmem_limit_bytes=WHOLE_VMEM),
        name="tail",
    )(q_nope, q_rope, w_uk, w_uv, suffix_t, suffix_len)


def combine_kernel(got_ref, tail_ref, tail_stats_ref, out_ref, got32, *, heads, sources):
    got32[...] = got_ref[...].astype(jnp.float32)
    stats = got32[pl.ds(heads, sources, stride=ROWS), :]

    def part(first, count):
        terms = [pltpu.roll(stats, (LANES - 16 * k) % LANES, 1) if k else stats for k in range(first, first + count)]
        return sum(terms[1:], terms[0])

    peak = part(0, 3)
    mass = part(3, 2)
    tail_peak = tail_stats_ref[0:1, :]
    tail_mass = tail_stats_ref[1:2, :]
    highest = jnp.maximum(jnp.max(peak, axis=0, keepdims=True), tail_peak)
    factor = jnp.exp2(peak - highest)
    tail_factor = jnp.exp2(tail_peak - highest)
    total = jnp.sum(factor * mass, axis=0, keepdims=True) + tail_factor * tail_mass
    lane = lax.broadcasted_iota(jnp.int32, total.shape, 1)
    total = jnp.where(lane < heads, total, 1.0)
    share = jnp.concatenate(
        [
            factor / total,
            jnp.broadcast_to(tail_factor / total, (8, LANES)),
            jnp.zeros((LANES - sources - 8, LANES), jnp.float32),
        ],
        axis=0,
    )
    share = share.T[:heads]
    value = tail_ref[...] * share[:, sources : sources + 1]
    for s in range(sources):
        value = value + got32[s * ROWS : s * ROWS + heads, :] * share[:, s : s + 1]
    value = value.astype(jnp.bfloat16)
    for s in range(sources):
        out_ref[s * heads : (s + 1) * heads, :] = value


def combine(got, tail, tail_stats, sources):
    heads = tail.shape[0]
    return pl.pallas_call(
        functools.partial(combine_kernel, heads=heads, sources=sources),
        out_shape=jax.ShapeDtypeStruct((sources * heads, LANES), jnp.bfloat16),
        in_specs=[pl.BlockSpec(memory_space=pltpu.VMEM)] * 3,
        out_specs=pl.BlockSpec(memory_space=pltpu.VMEM),
        scratch_shapes=[pltpu.VMEM((sources * ROWS, LANES), jnp.float32)],
        compiler_params=pltpu.CompilerParams(vmem_limit_bytes=8 * 1024 * 1024),
        name="combine",
    )(got, tail, tail_stats)


def output_kernel(values_ref, w_ref, out_ref, values32, flat, *, heads, requests, first):
    values32[...] = values_ref[...].astype(jnp.float32)
    for h in range(heads):
        value = values32[pl.ds(h, requests, stride=heads), :]
        flat[:, h * LANES : (h + 1) * LANES] = pltpu.roll(value, CTX_FIRST, 0).astype(jnp.bfloat16)
    product = lax.dot_general(
        flat[...], w_ref[...], (((1,), (1,)), ((), ())), preferred_element_type=jnp.float32
    )
    out_ref[: requests - first, :] = product[first:]
    out_ref[requests - first :, :] = product[:first]


def output_product(values, w_out_t, requests, first):
    heads = values.shape[0] // requests
    return pl.pallas_call(
        functools.partial(output_kernel, heads=heads, requests=requests, first=first),
        out_shape=jax.ShapeDtypeStruct((requests, w_out_t.shape[0]), jnp.float32),
        in_specs=[pl.BlockSpec(memory_space=pltpu.VMEM)] * 2,
        out_specs=pl.BlockSpec(memory_space=pltpu.VMEM),
        scratch_shapes=[
            pltpu.VMEM(values.shape, jnp.float32),
            pltpu.VMEM((requests, heads * LANES), jnp.bfloat16),
        ],
        compiler_params=pltpu.CompilerParams(vmem_limit_bytes=8 * 1024 * 1024),
        name="output_product",
    )(values, w_out_t)


def exchange(value, axis, first):
    count = lax.axis_size(axis)
    order = [[(k + first) % count for k in range(count)]]
    return lax.all_to_all(value, axis, 0, 0, axis_index_groups=order, tiled=True)


def on_device(
    q_nope,
    q_rope,
    w_uk,
    w_uv,
    w_out,
    prefix_cache,
    block_table,
    prefix_len,
    suffix_cache,
    suffix_len,
):
    requests = prefix_len.shape[0]
    heads = w_uk.shape[0]
    packed_query, positions, lens = pack(q_nope[0], q_rope[0], block_table, prefix_len)
    raw = exchange(packed_query, "ctx", CTX_FIRST)
    tail, tail_stats = tail_part(
        q_nope[0], q_rope[0], w_uk, w_uv, suffix_cache[0].T, suffix_len
    )
    raw, tail, tail_stats = lax.optimization_barrier((raw, tail, tail_stats))
    packed = segment(
        raw.reshape(requests * ROWS, LANES),
        w_uk,
        positions,
        lens,
        prefix_cache.T,
        w_uv,
    )
    got = exchange(packed.reshape(requests, ROWS, LANES), "ctx", CTX_FIRST)
    values = combine(got.reshape(requests * ROWS, LANES), tail, tail_stats, requests)
    every = exchange(values.reshape(requests, heads, LANES), "ctx", CTX_FIRST)
    tp = lax.axis_size("tp")
    first = TP_FIRST * (requests // tp)
    partial = output_product(every.reshape(requests * heads, LANES), w_out.T, requests, first)
    pieces = exchange(partial.reshape(tp, requests // tp, -1), "tp", TP_FIRST)
    return pieces.sum(axis=0).astype(jnp.bfloat16)


def solution(mesh):
    placed = (
        P("ctx", "tp", None),
        P("ctx", "tp", None),
        P("tp", None, None),
        P("tp", None, None),
        P("tp", "ctx"),
        P("ctx", None),
        P("ctx"),
        P(),
        P("ctx", None, None),
        P("ctx"),
    )
    return jax.shard_map(
        on_device, mesh=mesh, in_specs=placed, out_specs=P("tp", "ctx"), check_vma=False
    )
```
